32 devices in a mesh: grp: 8 (over y, x, core), seq: 4 (over z).
Axes of the slice: x: 2, y: 2, z: 4, core: 2. Of those that a mesh axis runs over, the one named last changes fastest.
Arguments:
- features: bfloat16 [8, 32, 64, 512], P('grp', 'seq'), may hold values from -6 to 6
- gn_gain: float32 [512], replicated, may hold values from 0.25 to 1.75
- gn_bias: float32 [512], replicated, may hold values from -3 to 3
- conv_weight: bfloat16 [8, 9, 512], replicated, may hold values from -0.09375 to 0.09375
- conv_bias: float32 [8], replicated, may hold values from -3 to 3
- quant_weight: float32 [4, 8], replicated, may hold values from -3 to 3
- quant_bias: float32 [4], replicated, may hold values from -3 to 3
- route: int32 [8], replicated, may hold values from 0 to 7, as said below
- bucket: int32 [8, 2], replicated, may hold values from 8 to 32, as said below
- times: float32 [8], P('grp'), may hold values from 0.05 to 0.95
- noise: float32 [8, 8192], P('grp'), may hold values from -6 to 6
- modulation: float32 [8, 2, 3072], P('grp'), may hold values from -3 to 3
- embed_weight: bfloat16 [16, 3072], replicated, may hold values from -1.5 to 1.5
- qkv_weight: bfloat16 [3072, 3, 512], P(None, None, 'seq'), may hold values from -1 to 1
Outputs:
- attended: bfloat16 [8, 512, 512], P('grp', 'seq')
The draws below stay inside these ranges and needn't reach their ends.
Inputs may be any that keep to these rules, and one draw needn't show every extreme that they name: `bucket`: column 0 is an image's height (at most 16, at least half of it) and column 1 its width (at most 32, at least half of it); some image fills both. `route`: each trainer group receives exactly one image; some image g goes to group (g + 4) mod 8.
All inputs are finite; a program needn't handle non-finite values.
Results may differ from the reference program's by a relative error of at most 0.011.
Values may be sent and summed in bfloat16 or wider, within the bound.
A program may use at most 128 MiB of HBM per device.

```python
import jax
import jax.numpy as jnp
from jax import lax

D = 3072
C = 512
HEAD = 128
PATCH_DIM = 16
PATCH_COLS = 32
HEADS = 4
PATCH_ROWS = 16
LAT_ROWS = 32
LAT_COLS = 64
SEQ_TOK = 512
IMAGES = 8


def draw_route(key, part):
    base = jax.random.fold_in(key, 41)
    first_key, second_key = jax.random.split(base, 2)
    shuffled = jax.random.permutation(first_key, IMAGES).astype(jnp.int32)
    chosen = jax.random.randint(second_key, (), 0, IMAGES).astype(jnp.int32)
    target = ((chosen + IMAGES // 2) % IMAGES).astype(jnp.int32)
    holder = jnp.argmax((shuffled == target).astype(jnp.int32)).astype(jnp.int32)
    previous = shuffled[chosen]
    positions = jnp.arange(IMAGES, dtype=jnp.int32)
    swapped = jnp.where(positions == holder, previous, shuffled)
    swapped = jnp.where(positions == chosen, target, swapped)
    return swapped.astype(jnp.int32)


def draw_bucket(key, part):
    base = jax.random.fold_in(key, 17)
    first_key, second_key, third_key = jax.random.split(base, 3)
    heights = jax.random.randint(first_key, (IMAGES,), PATCH_ROWS // 2, PATCH_ROWS + 1)
    breadths = jax.random.randint(second_key, (IMAGES,), PATCH_COLS // 2, PATCH_COLS + 1)
    filled = jax.random.randint(third_key, (), 0, IMAGES)
    chosen = jnp.arange(IMAGES) == filled
    heights = jnp.where(chosen, PATCH_ROWS, heights)
    breadths = jnp.where(chosen, PATCH_COLS, breadths)
    return jnp.stack([heights, breadths], axis=1).astype(jnp.int32)


def draw_qkv_weight(key, part):
    base = jax.random.fold_in(key, 29)
    first_key = jax.random.fold_in(base, 0)
    deviation = D ** (-0.5)
    columns = HEADS * HEAD
    drawn = jax.random.normal(first_key, (D, 3, columns), jnp.float32) * deviation
    return jnp.clip(drawn, -6.0 * deviation, 6.0 * deviation).astype(jnp.bfloat16)


def block_levels(own_key, shape, cuts, least, high):
    loudness, own = 1.0, jax.random.fold_in(own_key, 6)
    for dim, shards_of in cuts:
        draws = jnp.exp(jax.random.uniform(jax.random.fold_in(own, dim), (shards_of,), jnp.float32, least / len(cuts), high / len(cuts)))
        loudness = loudness * jnp.repeat(draws, shape[dim] // shards_of).reshape([-1 if axis == dim else 1 for axis in range(len(shape))])
    return loudness


def scatter_about(stream_key, shape, scale, reach, cuts=(), kind=jnp.bfloat16):
    loudness = block_levels(stream_key, shape, cuts, -0.22, 0.18) if cuts else 1.0
    values = jax.random.normal(stream_key, shape, jnp.float32) * scale * loudness
    return jnp.minimum(jnp.maximum(values, -reach), reach).astype(kind)


def setup_inputs(seed: int = 0) -> dict:
    seeds = jax.random.split(jax.random.key(seed), 15)
    features = scatter_about(seeds[0], (IMAGES, LAT_ROWS, LAT_COLS, C), 1.0, 6.0, ((0, 8), (1, 4)))
    gn_gain = jnp.clip(1.0 + 0.15 * jax.random.normal(seeds[1], (C,), jnp.float32), 0.25, 1.75)
    gn_bias = scatter_about(seeds[2], (C,), 0.5, 3.0, (), jnp.float32)
    conv_weight = scatter_about(seeds[3], (8, 9, C), (9 * C) ** -0.5, 0.09375)
    conv_bias = scatter_about(seeds[4], (8,), 0.5, 3.0, (), jnp.float32)
    quant_weight = scatter_about(seeds[5], (4, 8), 4 ** -0.5, 3.0, (), jnp.float32)
    quant_bias = scatter_about(seeds[6], (4,), 0.5, 3.0, (), jnp.float32)
    route = draw_route(jax.random.fold_in(seeds[14], 71), 0)
    bucket = draw_bucket(jax.random.fold_in(seeds[14], 71), 0)
    times = jnp.clip(0.05 + 0.9 * jax.random.uniform(seeds[9], (IMAGES,), jnp.float32) ** block_levels(seeds[9], (IMAGES,), ((0, 8),), -0.2, 0.2), 0.05, 0.95)
    noise = scatter_about(seeds[10], (IMAGES, SEQ_TOK * PATCH_DIM), 1.0, 6.0, ((0, 8),), jnp.float32)
    modulation = scatter_about(seeds[11], (IMAGES, 2, D), 0.5, 3.0, ((0, 8),), jnp.float32)
    embed_weight = scatter_about(seeds[12], (PATCH_DIM, D), PATCH_DIM ** -0.5, 1.5)
    qkv_weight = draw_qkv_weight(jax.random.fold_in(seeds[14], 71), 0)
    return dict(features=features, gn_gain=gn_gain, gn_bias=gn_bias, conv_weight=conv_weight, conv_bias=conv_bias, quant_weight=quant_weight, quant_bias=quant_bias, route=route, bucket=bucket, times=times, noise=noise, modulation=modulation, embed_weight=embed_weight, qkv_weight=qkv_weight)


epsilon = 1e-06

def position_table(row_index, col_index):
    quarter = D // 4
    frequency = 10000.0 ** (-jnp.arange(quarter, dtype=jnp.float32) / quarter)
    row_angle = row_index.astype(jnp.float32)[:, None] * frequency[None, :]
    col_angle = col_index.astype(jnp.float32)[:, None] * frequency[None, :]
    return jnp.concatenate([jnp.sin(row_angle), jnp.cos(row_angle), jnp.sin(col_angle), jnp.cos(col_angle)], axis=1)

def encode(feature_map, height, breadth, gn_gain, gn_bias, conv_weight, conv_bias, quant_weight, quant_bias):
    lat_rows, lat_cols, channels = feature_map.shape
    per_group = channels // 32
    valid_rows = jnp.arange(lat_rows) < 2 * height
    valid_cols = jnp.arange(lat_cols) < 2 * breadth
    inside = (valid_rows[:, None] & valid_cols[None, :]).astype(jnp.float32)
    inside_four = inside[:, :, None, None]
    grouped = feature_map.astype(jnp.float32).reshape(lat_rows, lat_cols, 32, per_group)
    pixel_count = (4 * height * breadth * per_group).astype(jnp.float32)
    group_mean = lax.optimization_barrier(jnp.sum(inside_four * grouped, axis=(0, 1, 3))) / pixel_count
    centered = grouped - group_mean[None, None, :, None]
    group_var = lax.optimization_barrier(jnp.sum(inside_four * centered * centered, axis=(0, 1, 3))) / pixel_count
    normed = (centered * lax.rsqrt(group_var + epsilon)[None, None, :, None]).reshape(lat_rows, lat_cols, channels)
    normed = normed * gn_gain + gn_bias
    hidden = (jax.nn.silu(normed) * inside[:, :, None]).astype(jnp.bfloat16)
    padded = jnp.pad(hidden, ((1, 1), (1, 1), (0, 0))).astype(jnp.float32)
    kernel = conv_weight.astype(jnp.float32)
    summed = jnp.zeros((8, lat_rows, lat_cols), jnp.float32)
    for offset in range(9):
        window = padded[offset // 3:offset // 3 + lat_rows, offset % 3:offset % 3 + lat_cols]
        summed = summed + jnp.einsum('rwc,oc->orw', window, kernel[:, offset, :])
    summed = summed + conv_bias[:, None, None]
    return jnp.einsum('ki,irw->krw', quant_weight, summed, precision=lax.Precision.HIGHEST) + quant_bias[:, None, None]

def embed_tokens(positions, patches, patch_cols, height, breadth, moment, noise_rows, modulation_row, embed_weight):
    live_tokens = positions < height * breadth
    row_index = positions // breadth
    col_index = positions % breadth
    source = jnp.where(live_tokens, row_index * patch_cols + col_index, 0).astype(jnp.int32)
    picked = jnp.take(patches, source, axis=0) * live_tokens[:, None].astype(jnp.float32)
    noisy = (1.0 - moment) * picked + moment * noise_rows
    embedded = jnp.dot(noisy.astype(jnp.bfloat16), embed_weight, preferred_element_type=jnp.float32)
    embedded = embedded + position_table(row_index, col_index)
    centre = embedded - lax.optimization_barrier(jnp.mean(embedded, axis=1, keepdims=True))
    spread = lax.optimization_barrier(jnp.mean(centre * centre, axis=1, keepdims=True))
    normed = centre * lax.rsqrt(spread + epsilon)
    return (normed * (1.0 + modulation_row[1]) + modulation_row[0]).astype(jnp.bfloat16)

def attend(query_rows, key_rows, value_rows, live_tokens):
    scores = jnp.dot(query_rows, key_rows.T, preferred_element_type=jnp.float32) * HEAD ** (-0.5)
    scores = jnp.where(live_tokens[None, :], scores, -jnp.inf)
    largest = lax.optimization_barrier(jnp.max(scores, axis=1, keepdims=True))
    powers = jnp.exp(scores - largest)
    probabilities = (powers / lax.optimization_barrier(jnp.sum(powers, axis=1, keepdims=True))).astype(jnp.bfloat16)
    return jnp.dot(probabilities, value_rows, preferred_element_type=jnp.float32).astype(jnp.bfloat16)

def reference(features, gn_gain, gn_bias, conv_weight, conv_bias, quant_weight, quant_bias, route, bucket, times, noise, modulation, embed_weight, qkv_weight):

    def encode_one(packed):
        return encode(packed[0], packed[1][0], packed[1][1], gn_gain, gn_bias, conv_weight, conv_bias, quant_weight, quant_bias)
    latents = lax.map(encode_one, (features, bucket))
    inverse = jnp.zeros((IMAGES,), jnp.int32).at[route].set(jnp.arange(IMAGES, dtype=jnp.int32))

    def train_one(trainer):
        source = inverse[trainer]
        latent = latents[source]
        height = bucket[source, 0]
        breadth = bucket[source, 1]
        patch_rows = latent.shape[1] // 2
        patch_cols = latent.shape[2] // 2
        patches = latent.reshape(4, patch_rows, 2, patch_cols, 2).transpose(1, 3, 0, 2, 4).reshape(patch_rows * patch_cols, 16)
        positions = jnp.arange(SEQ_TOK, dtype=jnp.int32)
        tokens = embed_tokens(positions, patches, patch_cols, height, breadth, times[trainer], noise[trainer].reshape(SEQ_TOK, 16), modulation[trainer], embed_weight)
        projected = jnp.einsum('td,dkh->kth', tokens.astype(jnp.float32), qkv_weight.astype(jnp.float32)).astype(jnp.bfloat16)
        split_heads = projected.reshape(3, SEQ_TOK, HEADS, HEAD).transpose(0, 2, 1, 3)
        live_tokens = positions < height * breadth

        def one_head(triple):
            return attend(triple[0], triple[1], triple[2], live_tokens)
        outputs = lax.map(one_head, (split_heads[0], split_heads[1], split_heads[2]))
        joined = outputs.transpose(1, 0, 2).reshape(SEQ_TOK, HEADS * HEAD)
        return joined * live_tokens[:, None].astype(jnp.bfloat16)
    return lax.map(train_one, jnp.arange(IMAGES, dtype=jnp.int32))
```

```python
import functools

import numpy as np
import jax
import jax.numpy as jnp
from jax import lax
from jax.experimental import pallas as pl
from jax.experimental.pallas import tpu as pltpu
from jax.sharding import PartitionSpec as P

HEAD = 128
GROUPS = 32
PATCH = 16
EPS = 1e-06
MESH = pl.DeviceIdType.MESH
F32 = jnp.float32
BF16 = jnp.bfloat16
HIGHEST = lax.Precision.HIGHEST


def iota(shape, dim):
    return lax.broadcasted_iota(jnp.int32, shape, dim)


def one(cond, dtype=F32):
    return jnp.where(cond, 1.0, 0.0).astype(dtype)


def split2(x):
    hi = x.astype(BF16)
    return hi, (x - hi.astype(F32)).astype(BF16)


def split3(x):
    hi = x.astype(BF16)
    rest = x - hi.astype(F32)
    mid, low = split2(rest)
    return hi, mid, low


def mm(a, b, precision=None):
    return jnp.dot(a, b, preferred_element_type=F32, precision=precision)


def mm_nt(a, b):
    return lax.dot_general(a, b, (((1,), (1,)), ((), ())), preferred_element_type=F32)


def select3(x, chosen):
    hi, mid, low = split3(x)
    return mm(hi, chosen) + mm(mid, chosen) + mm(low, chosen)


def position_rows(rows, cols, width):
    quarter = width // 4
    freq = (np.float32(10000.0) ** (-np.arange(quarter, dtype=np.float32) / np.float32(quarter))).astype(np.float32)
    table = np.zeros((rows + cols, width), np.float64)
    for start, count, base in ((0, rows, 0), (rows, cols, 2 * quarter)):
        angle = (np.arange(count, dtype=np.float32)[:, None] * freq[None, :]).astype(np.float64)
        table[start : start + count, base : base + quarter] = np.sin(angle)
        table[start : start + count, base + quarter : base + 2 * quarter] = np.cos(angle)
    table = table - table.mean(axis=1, keepdims=True)
    return table.astype(np.float32)


def kernel(
    n,
    g,
    dims,
    route_hbm,
    bucket_hbm,
    times_hbm,
    feat_hbm,
    w_hbm,
    table_hbm,
    gain_hbm,
    gbias_hbm,
    conv_hbm,
    cbias_hbm,
    quant_hbm,
    qbias_hbm,
    noise_hbm,
    mod_hbm,
    embed_hbm,
    out_ref,
    route_ref,
    bucket_ref,
    times_ref,
    feat,
    w_ref,
    table,
    gain_ref,
    gbias_ref,
    conv_ref,
    cbias_ref,
    quant_ref,
    qbias_ref,
    noise_ref,
    mod_ref,
    embed_ref,
    xperm,
    stats,
    lat,
    gath,
    bw_all,
    bwt,
    bc,
    bs,
    at,
    pick,
    local_sem,
    st_send,
    st_recv,
    lat_send,
    lat_recv,
    ga_send,
    ga_recv,
    bw_send,
    bw_recv,
):
    strip_rows, lat_cols, chans, seq_tokens, width = dims
    cells = strip_rows * lat_cols
    plane = cells // 4
    half = lat_cols // 2
    prow = strip_rows // 2
    patch_rows = prow * n
    kr = PATCH + patch_rows + half
    kb = kr + 16
    per_group = chans // GROUPS
    me = lax.axis_index("seq")
    t = lax.axis_index("grp")

    hbm = (
        feat_hbm, bucket_hbm, route_hbm, times_hbm, table_hbm, embed_hbm, mod_hbm, w_hbm,
        gain_hbm, gbias_hbm, conv_hbm, cbias_hbm, quant_hbm, qbias_hbm, noise_hbm,
    )
    local = (
        feat, bucket_ref, route_ref, times_ref, table, embed_ref, mod_ref, w_ref,
        gain_ref, gbias_ref, conv_ref, cbias_ref, quant_ref, qbias_ref, noise_ref,
    )
    loads = [pltpu.make_async_copy(a, b, local_sem.at[i]) for i, (a, b) in enumerate(zip(hbm, local))]
    for copy in loads[:2]:
        copy.start()

    barrier = pltpu.get_barrier_semaphore()
    for o in range(1, n):
        pl.semaphore_signal(barrier, inc=1, device_id={"seq": lax.rem(me + o, n)}, device_id_type=MESH)
    for o in range(1, g):
        pl.semaphore_signal(barrier, inc=1, device_id={"grp": lax.rem(t + o, g)}, device_id_type=MESH)

    for copy in loads[2:]:
        copy.start()

    def exchange(buf, send_sem, recv_sem, axis, mine, size):
        return [
            pltpu.make_async_remote_copy(
                src_ref=buf.at[mine],
                dst_ref=buf.at[mine],
                send_sem=send_sem.at[o],
                recv_sem=recv_sem.at[o],
                device_id={axis: lax.rem(mine + o, size)},
                device_id_type=MESH,
            )
            for o in range(1, size)
        ]

    ex_stats = exchange(stats, st_send, st_recv, "seq", me, n)
    ex_lat = exchange(lat, lat_send, lat_recv, "grp", t, g)
    ex_gath = exchange(gath, ga_send, ga_recv, "seq", me, n)
    ex_bw = exchange(bw_all, bw_send, bw_recv, "seq", me, n)

    loads[1].wait()
    height = bucket_ref[0, t]
    breadth = bucket_ref[1, t]
    cell = iota((cells, 1), 0)
    valid = ((cell // lat_cols + me * strip_rows) < 2 * height) & ((cell % lat_cols) < 2 * breadth)
    inside = one(valid)

    def inside_count(strip):
        rows = jnp.clip(2 * height - strip * strip_rows, 0, strip_rows)
        return (rows * 2 * breadth).astype(F32)

    loads[0].wait()
    x = feat[...].astype(F32)
    total = jnp.sum(x * inside, axis=0, keepdims=True)
    own = jnp.maximum(inside_count(me), 1.0)
    centred = (x - total / own) * inside
    second = jnp.sum(centred * centred, axis=0, keepdims=True)
    stats[me] = jnp.concatenate([total, second], axis=0)
    pl.semaphore_wait(barrier, n - 1 + g - 1)
    for copy in ex_stats:
        copy.start()

    order = iota((cells, cells), 0)
    ab, inner = order // plane, order % plane
    origin = (2 * (inner // half) + ab // 2) * lat_cols + 2 * (inner % half) + ab % 2
    perm = one(iota((cells, cells), 1) == origin, BF16)
    xperm[...] = mm(perm, feat[...]).astype(BF16)
    new = iota((cells, 1), 0)
    nab, ninner = new // plane, new % plane
    nrow = 2 * (ninner // half) + nab // 2 + me * strip_rows
    ncol = 2 * (ninner % half) + nab % 2
    inside_perm = one((nrow < 2 * height) & (ncol < 2 * breadth))
    same = one(iota((chans, chans), 0) // per_group == iota((chans, chans), 1) // per_group, BF16)

    for copy in loads[4:7]:
        copy.wait()
    scale = 1.0 + mod_ref[1:2, :]
    shift = mod_ref[0:1, :]
    for i in range(kr // 16):
        if i == 0:
            block = embed_ref[...].astype(F32)
            block = block - jnp.mean(block, axis=1, keepdims=True)
        else:
            block = table[16 * (i - 1) : 16 * i, :]
        hi, low = split2(block)
        bc[16 * i : 16 * i + 16, :] = hi
        bc[kr + 16 * i : kr + 16 * i + 16, :] = low
        hi, low = split2(block * scale)
        bs[16 * i : 16 * i + 16, :] = hi
        bs[kb + 16 * i : kb + 16 * i + 16, :] = low
    hi, low = split2(jnp.where(iota((16, width), 0) == 0, shift, 0.0))
    bs[kr:kb, :] = hi
    bs[kb + kr : 2 * kb, :] = low
    loads[7].wait()
    for i in range(3):
        both = mm(bs[...], w_ref[i])
        bw_all[me, :, i * HEAD : (i + 1) * HEAD] = (both[:kb] + both[kb:]).astype(BF16)
    for copy in ex_bw:
        copy.start()

    for copy in loads[2:4] + loads[8:]:
        copy.wait()
    for copy in ex_stats:
        copy.wait_recv()
    pixels = (4 * height * breadth * per_group).astype(F32)
    sums = [stats[i] for i in range(n)]
    channel_sum = sums[0][0:1]
    for i in range(1, n):
        channel_sum = channel_sum + sums[i][0:1]
    eight = jnp.zeros((8, chans), F32)
    mean = select3(channel_sum + eight, same)[0:1] / pixels
    squares = jnp.zeros((1, chans), F32)
    for i in range(n):
        count = inside_count(i)
        away = sums[i][0:1] / jnp.maximum(count, 1.0) - mean
        squares = squares + sums[i][1:2] + count * away * away
    var = select3(squares + eight, same)[0:1] / pixels
    slope = lax.rsqrt(var + EPS) * gain_ref[...]
    y = (xperm[...].astype(F32) - mean) * slope + gbias_ref[...]
    y = y * (0.5 * jnp.tanh(0.5 * y) + 0.5) * inside_perm
    hidden = y.astype(BF16)

    taps = mm_nt(conv_ref[...], hidden)
    lane = iota((8, plane), 1)
    lane_q, lane_p = lane % half, lane // half

    def piece(dy, dx, a, b):
        k = 3 * dy + dx
        p = 2 * a + b
        return taps[8 * k : 8 * k + 8, p * plane : (p + 1) * plane]

    def across(dy, a, b):
        z = piece(dy, 1, a, b)
        if b == 0:
            prev = pltpu.roll(piece(dy, 0, a, 1), 1, axis=1)
            return z + jnp.where(lane_q == 0, 0.0, prev) + piece(dy, 2, a, 1)
        after = pltpu.roll(piece(dy, 2, a, 0), plane - 1, axis=1)
        return z + piece(dy, 0, a, 0) + jnp.where(lane_q == half - 1, 0.0, after)

    inner_planes, edge_planes = [], []
    for a in range(2):
        for b in range(2):
            z = across(1, a, b)
            if a == 0:
                moved = pltpu.roll(across(0, 1, b), half, axis=1)
                edge = lane_p == 0
                z = z + across(2, 1, b)
            else:
                moved = pltpu.roll(across(2, 0, b), plane - half, axis=1)
                edge = lane_p == prow - 1
                z = z + across(0, 0, b)
            inner_planes.append(z + jnp.where(edge, 0.0, moved))
            edge_planes.append(jnp.where(edge, moved, 0.0))
    stacked = jnp.concatenate(
        [jnp.concatenate(inner_planes, axis=0), jnp.concatenate(edge_planes, axis=0)], axis=1
    )
    pick_k = one(iota((PATCH, 4), 0) // 4 == iota((PATCH, 4), 1))
    quant_rows = mm(pick_k, quant_ref[...], HIGHEST)
    tile_o = one(iota((8, 32), 1) % 8 == iota((8, 32), 0))
    spread_q = mm(quant_rows, tile_o, HIGHEST)
    spread_q = jnp.where(iota((PATCH, 32), 0) % 4 == iota((PATCH, 32), 1) // 8, spread_q, 0.0)
    lat[t] = mm(spread_q, stacked, HIGHEST)
    for copy in ex_lat:
        copy.start()

    bias = jnp.sum(quant_rows * cbias_ref[...], axis=1, keepdims=True) + jnp.sum(
        pick_k * qbias_ref[...], axis=1, keepdims=True
    )
    source = jnp.int32(0)
    for i in range(g):
        source = jnp.where(route_ref[i] == t, i, source)
    tall = bucket_ref[0, source]
    wide = bucket_ref[1, source]
    alive_count = tall * wide
    token = iota((1, seq_tokens), 1)
    wide_f = jnp.full((1, seq_tokens), wide.astype(F32))
    row_f = jnp.floor((token.astype(F32) + 0.5) / wide_f)
    col_f = token.astype(F32) - row_f * wide_f
    row_i, col_i = row_f.astype(jnp.int32), col_f.astype(jnp.int32)
    alive = token < alive_count
    at[PATCH : PATCH + patch_rows, :] = one(iota((patch_rows, seq_tokens), 0) == row_i, BF16)
    at[PATCH + patch_rows : kr, :] = one(iota((half, seq_tokens), 0) == col_i, BF16)
    wanted = jnp.where(alive, row_i * half + col_i, -1)
    for i in range(n):
        pick[i * plane : (i + 1) * plane, :] = one(iota((plane, seq_tokens), 0) + i * plane == wanted, BF16)
    flat = noise_ref[...].T
    lines = seq_tokens * PATCH // 128
    noise_t = jnp.zeros((PATCH, seq_tokens), F32)
    where_line = iota((lines, seq_tokens), 0)
    where_token = iota((lines, seq_tokens), 1)
    for m in range(128 // PATCH):
        chosen = one(where_token == where_line * (128 // PATCH) + m, BF16)
        hi, low = split2(flat[PATCH * m : PATCH * m + PATCH, :])
        noise_t = noise_t + mm(hi, chosen) + mm(low, chosen)
    moment = times_ref[0]
    noise_t = noise_t * moment
    gram = mm_nt(bc[...], bc[...])
    gram = (gram[:kr, :kr] + gram[:kr, kr:] + gram[kr:, :kr] + gram[kr:, kr:]) * (1.0 / width)
    gram_hi, gram_low = split2(gram)

    for copy in ex_lat:
        copy.wait_recv()
    gath[me] = lat[source]
    for copy in ex_gath:
        copy.start()
    for copy in ex_bw:
        copy.wait_recv()
    for i in range(n):
        bwt[i] = bw_all[i].astype(F32).T.astype(BF16)
    for copy in ex_gath:
        copy.wait_recv()

    parts = [gath[i] for i in range(n)]
    upper = iota((PATCH, plane), 0) // 2 % 2 == 0
    pieces = []
    none = jnp.zeros((PATCH, plane), F32)
    for i in range(n):
        before = parts[i - 1][:, plane:] if i > 0 else none
        after = parts[i + 1][:, plane:] if i < n - 1 else none
        pieces.append(parts[i][:, :plane] + jnp.where(upper, before, after) + bias)
    patches = jnp.concatenate(pieces, axis=1)
    picked = select3(patches, pick[...])
    at[0:PATCH, :] = ((1.0 - moment) * picked + noise_t).astype(BF16)
    a_all = at[...]
    through = mm(gram_hi, a_all) + mm(gram_low, a_all)
    spread = jnp.sum(through * a_all.astype(F32), axis=0, keepdims=True)
    rstd = lax.rsqrt(jnp.maximum(spread, 0.0) + EPS)

    own_tokens = seq_tokens // n
    a_own = at[:, pl.ds(pl.multiple_of(me * own_tokens, own_tokens), own_tokens)]
    through_own = mm(gram_hi, a_own) + mm(gram_low, a_own)
    spread_own = jnp.sum(through_own * a_own.astype(F32), axis=0, keepdims=True)
    rstd_own = lax.rsqrt(jnp.maximum(spread_own, 0.0) + EPS)
    query_alive = (iota((own_tokens, 1), 0) + me * own_tokens) < alive_count
    for h in range(n):
        weights = bwt[h]
        biases = weights[:, kr : kr + 1].astype(F32)
        q_t = mm(weights[:HEAD, :kr], a_own) * rstd_own + biases[:HEAD]
        kv_t = mm(weights[HEAD:, :kr], a_all) * rstd + biases[HEAD:]
        kv_t = kv_t.astype(BF16)
        query = q_t.T.astype(BF16)
        scores = mm(query, kv_t[:HEAD]) * HEAD ** (-0.5)
        scores = jnp.where(alive, scores, -jnp.inf)
        powers = jnp.exp(scores - jnp.max(scores, axis=1, keepdims=True))
        probabilities = (powers * (1.0 / jnp.sum(powers, axis=1, keepdims=True))).astype(BF16)
        attended = mm_nt(probabilities, kv_t[HEAD:])
        out_ref[:, h * HEAD : (h + 1) * HEAD] = jnp.where(query_alive, attended, 0.0).astype(BF16)

    for copies in (ex_stats, ex_bw, ex_lat, ex_gath):
        for copy in copies:
            copy.wait_send()


def solution(mesh):
    n, g = mesh.shape["seq"], mesh.shape["grp"]

    def per_device(
        features,
        gn_gain,
        gn_bias,
        conv_weight,
        conv_bias,
        quant_weight,
        quant_bias,
        route,
        bucket,
        times,
        noise,
        modulation,
        embed_weight,
        qkv_weight,
    ):
        _, strip_rows, lat_cols, chans = features.shape
        width = embed_weight.shape[1]
        seq_tokens = noise.shape[1] // PATCH
        cells = strip_rows * lat_cols
        half = lat_cols // 2
        patch_rows = strip_rows // 2 * n
        plane = cells // 4
        kr = PATCH + patch_rows + half
        kb = kr + 16
        table = jnp.asarray(position_rows(patch_rows, half, width))
        dims = (strip_rows, lat_cols, chans, seq_tokens, width)
        vmem = pl.BlockSpec(memory_space=pltpu.VMEM)
        anywhere = pl.BlockSpec(memory_space=pl.ANY)
        dma = pltpu.SemaphoreType.DMA
        result = pl.pallas_call(
            functools.partial(kernel, n, g, dims),
            out_shape=pltpu.VMEM((seq_tokens // n, n * HEAD), BF16),
            in_specs=[anywhere] * 15,
            out_specs=vmem,
            scratch_shapes=[
                pltpu.SMEM(route.shape, jnp.int32),
                pltpu.SMEM(bucket.shape[::-1], jnp.int32),
                pltpu.SMEM(times.shape, F32),
                pltpu.VMEM((cells, chans), BF16),
                pltpu.VMEM((3, width, HEAD), BF16),
                pltpu.VMEM((patch_rows + half, width), F32),
                pltpu.VMEM((1, chans), F32),
                pltpu.VMEM((1, chans), F32),
                pltpu.VMEM((9 * conv_weight.shape[0], chans), BF16),
                pltpu.VMEM((1, conv_bias.shape[0]), F32),
                pltpu.VMEM(quant_weight.shape, F32),
                pltpu.VMEM((1, quant_bias.shape[0]), F32),
                pltpu.VMEM((noise.shape[1] // 128, 128), F32),
                pltpu.VMEM(modulation.shape[1:], F32),
                pltpu.VMEM(embed_weight.shape, BF16),
                pltpu.VMEM((cells, chans), BF16),
                pltpu.VMEM((n, 2, chans), F32),
                pltpu.VMEM((g, PATCH, 2 * plane), F32),
                pltpu.VMEM((n, PATCH, 2 * plane), F32),
                pltpu.VMEM((n, kb, 3 * HEAD), BF16),
                pltpu.VMEM((n, 3 * HEAD, kb), BF16),
                pltpu.VMEM((2 * kr, width), BF16),
                pltpu.VMEM((2 * kb, width), BF16),
                pltpu.VMEM((kr, seq_tokens), BF16),
                pltpu.VMEM((n * plane, seq_tokens), BF16),
                dma((15,)),
                dma((n,)),
                dma((n,)),
                dma((g,)),
                dma((g,)),
                dma((n,)),
                dma((n,)),
                dma((n,)),
                dma((n,)),
            ],
            compiler_params=pltpu.CompilerParams(
                collective_id=0, has_side_effects=True, vmem_limit_bytes=56 << 20
            ),
        )(
            route,
            bucket.T,
            times,
            features.reshape(cells, chans),
            qkv_weight.transpose(1, 0, 2),
            table,
            gn_gain.reshape(1, chans),
            gn_bias.reshape(1, chans),
            conv_weight.transpose(1, 0, 2).reshape(-1, chans),
            conv_bias.reshape(1, -1),
            quant_weight,
            quant_bias.reshape(1, -1),
            noise.reshape(-1, 128),
            modulation[0],
            embed_weight,
        )
        return result[None]

    in_specs = (
        P("grp", "seq", None, None),
        P(),
        P(),
        P(),
        P(),
        P(),
        P(),
        P(),
        P(),
        P("grp"),
        P("grp", None),
        P("grp", None, None),
        P(),
        P(None, None, "seq"),
    )
    return jax.shard_map(
        per_device, mesh=mesh, in_specs=in_specs, out_specs=P("grp", "seq", None), check_vma=False
    )
```
